512 devices in a mesh: grp: 2 (over y_hi), ctx: 32 (over z, core), dp: 8 (over x, y_lo).
Axes of the slice: x: 4, y: 4 (y_hi: 2, y_lo: 2; y = y_hi * 2 + y_lo), z: 16, core: 2. Of those that a mesh axis runs over, the one named last changes fastest.
Arguments:
- resid: bfloat16 [8, 4096, 1024], P('dp', 'ctx'), may hold values from -6 to 6
- attn_ctx: bfloat16 [8, 4096, 1024], P('dp', 'ctx', 'grp'), may hold values from -6 to 6
- enc_out_weight: bfloat16 [1024, 1024], P('grp'), may hold values from -0.1875 to 0.1875
- enc_gain: bfloat16 [1024], replicated, may hold values from 0.25 to 1.75
- key_weight: bfloat16 [1024, 1024], P(None, 'grp'), may hold values from -0.1875 to 0.1875
- value_weight: bfloat16 [1024, 1024], P(None, 'grp'), may hold values from -0.1875 to 0.1875
- visual_grad: bfloat16 [8, 4096, 1024], P('dp', 'ctx'), may hold values from -6 to 6
- scene_lengths: int32 [8, 4], P('dp'), may hold values from 1 to 1536, 4096 in all within a row
- text_queries: bfloat16 [8, 5120, 4096], P('dp', 'ctx', 'grp'), may hold values from -86 to 86
- text_segments: int32 [8, 5120], P('dp', 'ctx'), may hold values from 0 to 7, never falling along the last dimension, each value on 1 to 1280 neighbouring positions
- doc_scene: int32 [8, 8], P('dp'), may hold values from 0 to 3
Outputs:
- cross_context: bfloat16 [8, 5120, 4096], P('dp', 'ctx', 'grp')
- enc_out_grad: float32 [1024, 1024], P(('grp', 'ctx'))
The draws below stay inside these ranges and needn't reach their ends.
Inputs may be any that keep to these rules, and one draw needn't show every extreme that they name: `scene_lengths`: each replica's counts sum to 4096; the largest is exactly the maximum. `text_segments`: never falling along a sequence.
All inputs are finite; a program needn't handle non-finite values.
Results may differ from the reference program's by a relative error of at most 0.025.
Values may be sent and summed in bfloat16 or wider, within the bound.
No kernel may reach another device: no remote copies, remote signals or barrier semaphores. Data moves between devices by JAX's collectives and lax.ppermute only.
A program may use at most 64 MiB of HBM per device.

```python
import math
import jax
import jax.numpy as jnp
import numpy as np
from jax import lax

D_ENC = 1024
Q_HEADS = 32
KV_HEADS = 8
HEAD_DIM = 128
SCENES = 4
DOCS = 8
ENC_TOKENS = 4096
TEXT_TOKENS = 5120
N_DP = 8


def draw_text_queries(key, part):
    first_key = jax.random.fold_in(jax.random.fold_in(key, 17), 0)
    shape = (N_DP, TEXT_TOKENS, Q_HEADS * HEAD_DIM)
    values = jnp.clip(jax.random.normal(first_key, shape, jnp.float32), -6.0, 6.0)
    return values.astype(jnp.bfloat16)


def with_ends(drawn, rng, least, top_value):
    longest = drawn.shape.index(max(drawn.shape))
    spots = []
    for shift in (0, 1):
        where = [jax.random.randint(jax.random.fold_in(rng, axis), (), 0, length) for axis, length in enumerate(drawn.shape)]
        where[longest] = (where[longest] + shift) % drawn.shape[longest]
        spots.append(tuple(where))
    return drawn.at[spots[0]].set(least).at[spots[1]].set(top_value)


def with_spikes(drawn, key, source, target, blocks, factor):
    def block_of(dim):
        return (jnp.arange(drawn.shape[dim]) // (drawn.shape[dim] // blocks)).reshape((-1,) + (1,) * (drawn.ndim - 1 - dim))

    near = jax.random.permutation(key, blocks)[block_of(target)]
    other_side = (block_of(target) + blocks // 2) % blocks
    return jnp.where((block_of(source) == near) | (block_of(source) == other_side), factor * drawn, drawn)


def level_of(key, dims, cuts, least, high):
    def one(dim, parts):
        draws = jax.random.uniform(jax.random.fold_in(jax.random.fold_in(key, 6), dim), (parts,), jnp.float32, least / len(cuts), high / len(cuts))
        return jnp.repeat(jnp.exp(draws), dims[dim] // parts).reshape((-1,) + (1,) * (len(dims) - dim - 1))

    loudness = one(*cuts[0])
    for cut in cuts[1:]:
        loudness = loudness * one(*cut)
    return loudness


def length_profile(amount, total, bound, lean):
    loads = [(1 << 20) // math.isqrt(standing ** lean) + 1 for standing in range(2, amount + 1)]
    surplus, given = total - bound - (amount - 1), [1] * (amount - 1)
    while surplus > 0:
        movable = [i for i in range(amount - 1) if given[i] < bound]
        whole, remaining = sum([loads[i] for i in movable]), surplus
        for i in movable:
            more = min(bound - given[i], max(1, remaining * loads[i] // whole), surplus)
            given[i] = given[i] + more
            surplus = surplus - more
    return np.array([bound] + given)


def uneven_parts(stream_key, number_of, total, limit, skew):
    if number_of == 2:
        one = jax.random.randint(stream_key, (), max(1, total - limit), min(limit, total - 1) + 1)
        return jnp.stack([one, total - one])
    sizes = jnp.asarray(length_profile(number_of, total, limit, skew), jnp.int32)
    pairs = (number_of - 1) // 2
    donor, sink = sizes[1:1 + 2 * pairs:2], sizes[2:2 + 2 * pairs:2]
    margin = jnp.minimum(donor - 1, limit - sink)
    moved = jax.random.randint(jax.random.fold_in(stream_key, 1), (pairs,), 0, 1 << 20) % (margin + 1)
    sizes = sizes.at[1:1 + 2 * pairs:2].set(donor - moved).at[2:2 + 2 * pairs:2].set(sink + moved)
    return sizes[jax.random.permutation(jax.random.fold_in(stream_key, 2), number_of)]


def bell_draw(key, shape, width, limit, cuts=(), kind=jnp.bfloat16):
    values = jax.random.normal(key, shape, jnp.float32) * width
    if len(cuts) > 0:
        values = level_of(key, shape, cuts, -0.22, 0.18) * values
    return jnp.clip(values, min=-limit, max=limit).astype(kind)


def heavy_noise(key, extent, spread, most, pieces, heavy, kind=jnp.bfloat16):
    drawn = spread * jax.random.normal(key, extent, jnp.float32)
    if pieces:
        drawn = drawn * level_of(key, extent, pieces, -0.22, 0.18)
    return jnp.clip(with_spikes(drawn, jax.random.fold_in(key, 3), *heavy), -most, most).astype(kind)


def setup_inputs(seed: int = 0) -> dict:
    key_list = jax.random.split(jax.random.key(seed), 12)
    resid = bell_draw(key_list[0], (N_DP, ENC_TOKENS, D_ENC), 1.0, 6.0, ((0, 8), (1, 32)))
    attn_ctx = heavy_noise(key_list[1], (N_DP, ENC_TOKENS, D_ENC), 1.0, 6.0, ((0, 8), (1, 32), (2, 2)), (1, 2, 32, 2.75))
    enc_out_weight = bell_draw(key_list[2], (D_ENC, D_ENC), D_ENC ** -0.5, 0.1875, ((0, 2),))
    enc_gain = jnp.clip(1.0 + 0.15 * jax.random.normal(key_list[3], (D_ENC,), jnp.float32), 0.25, 1.75).astype(jnp.bfloat16)
    key_weight = bell_draw(key_list[4], (D_ENC, KV_HEADS * HEAD_DIM), D_ENC ** -0.5, 0.1875, ((1, 2),))
    value_weight = bell_draw(key_list[5], (D_ENC, KV_HEADS * HEAD_DIM), D_ENC ** -0.5, 0.1875, ((1, 2),))
    visual_grad = bell_draw(key_list[6], (N_DP, ENC_TOKENS, D_ENC), 1.0, 6.0, ((0, 8), (1, 32)))
    scene_lengths = jax.vmap(lambda own: uneven_parts(own, SCENES, ENC_TOKENS, ENC_TOKENS * 3 // 8, 2))(jax.random.split(key_list[7], N_DP)).reshape((N_DP, SCENES)).astype(jnp.int32)
    text_queries = draw_text_queries(jax.random.fold_in(key_list[11], 71), 0)
    text_segments = jax.vmap(lambda own: jnp.searchsorted(jnp.cumsum(uneven_parts(own, DOCS, TEXT_TOKENS, TEXT_TOKENS // 4, 2)), jnp.arange(TEXT_TOKENS), side="right"))(jax.random.split(key_list[9], N_DP)).reshape((N_DP, TEXT_TOKENS)).astype(jnp.int32)
    doc_scene = with_ends(jax.random.randint(key_list[10], (N_DP, DOCS), 0, SCENES), jax.random.fold_in(key_list[10], 1), 0, SCENES - 1).astype(jnp.int32)
    return dict(resid=resid, attn_ctx=attn_ctx, enc_out_weight=enc_out_weight, enc_gain=enc_gain, key_weight=key_weight, value_weight=value_weight, visual_grad=visual_grad, scene_lengths=scene_lengths, text_queries=text_queries, text_segments=text_segments, doc_scene=doc_scene)


NEGATIVE = -1e+30
EPSILON = 1e-05

def scene_index(lengths, first_row, count):
    scene_ends = jnp.cumsum(lengths)
    position = first_row + jnp.arange(count, dtype=jnp.int32)
    return lax.optimization_barrier(jnp.sum((position[:, None] >= scene_ends[None, :]).astype(jnp.int32), axis=1))

def query_scenes(segments, doc_scene):
    doc_numbers = jnp.arange(doc_scene.shape[0], dtype=jnp.int32)
    picked = (segments[:, None] == doc_numbers[None, :]).astype(jnp.int32)
    return lax.optimization_barrier(jnp.sum(picked * doc_scene[None, :], axis=1))

def normalize(hidden, enc_gain):
    root_mean = jnp.sqrt(lax.optimization_barrier(jnp.mean(hidden * hidden, axis=-1, keepdims=True)) + EPSILON)
    normed = hidden / root_mean
    visual = (normed * enc_gain.astype(jnp.float32)).astype(jnp.bfloat16)
    return (normed, root_mean, visual)

def norm_backward(cotangent, normed, root_mean, enc_gain):
    upstream = cotangent.astype(jnp.float32) * enc_gain.astype(jnp.float32)
    inner = lax.optimization_barrier(jnp.mean(upstream * normed, axis=-1, keepdims=True))
    return ((upstream - normed * inner) / root_mean).astype(jnp.bfloat16)

def attend(queries, key_rows, value_rows, query_scene, key_scene):
    group_size = Q_HEADS // KV_HEADS
    allowed = query_scene[:, None] == key_scene[None, :]

    def one_head(head_index):
        kv_index = head_index // group_size
        query_block = lax.dynamic_slice_in_dim(queries, head_index * HEAD_DIM, HEAD_DIM, 1)
        key_block = lax.dynamic_slice_in_dim(key_rows, kv_index * HEAD_DIM, HEAD_DIM, 1)
        value_block = lax.dynamic_slice_in_dim(value_rows, kv_index * HEAD_DIM, HEAD_DIM, 1)
        scores = jnp.dot(query_block, key_block.T, preferred_element_type=jnp.float32) * HEAD_DIM ** (-0.5)
        scores = jnp.where(allowed, scores, NEGATIVE)
        largest = lax.optimization_barrier(jnp.max(scores, axis=1, keepdims=True))
        weights = jnp.where(allowed, jnp.exp(scores - largest), 0.0).astype(jnp.bfloat16)
        totals = lax.optimization_barrier(jnp.sum(weights.astype(jnp.float32), axis=1, keepdims=True))
        result = jnp.dot(weights, value_block, preferred_element_type=jnp.float32) / totals
        return result.astype(jnp.bfloat16)
    stacked = lax.map(one_head, jnp.arange(Q_HEADS, dtype=jnp.int32))
    return jnp.transpose(stacked, (1, 0, 2)).reshape(queries.shape[0], Q_HEADS * HEAD_DIM)

def reference(resid, attn_ctx, enc_out_weight, enc_gain, key_weight, value_weight, visual_grad, scene_lengths, text_queries, text_segments, doc_scene):

    def replica(index):
        hidden = resid[index].astype(jnp.float32) + jnp.dot(attn_ctx[index], enc_out_weight, preferred_element_type=jnp.float32)
        normed, root_mean, visual = normalize(hidden, enc_gain)
        key_rows = jnp.dot(visual, key_weight, preferred_element_type=jnp.float32).astype(jnp.bfloat16)
        value_rows = jnp.dot(visual, value_weight, preferred_element_type=jnp.float32).astype(jnp.bfloat16)
        hidden_grad = norm_backward(visual_grad[index], normed, root_mean, enc_gain)
        weight_term = jnp.dot(attn_ctx[index].T, hidden_grad, preferred_element_type=jnp.float32)
        key_scene = scene_index(scene_lengths[index], jnp.int32(0), ENC_TOKENS)
        query_scene = query_scenes(text_segments[index], doc_scene[index])
        context = attend(text_queries[index], key_rows, value_rows, query_scene, key_scene)
        return (context, weight_term)
    contexts, weight_terms = lax.map(replica, jnp.arange(N_DP, dtype=jnp.int32))
    return (contexts, lax.optimization_barrier(jnp.sum(weight_terms, axis=0)))
```

```python
import functools

import jax
import jax.numpy as jnp
from jax import lax
from jax.experimental import pallas as pl
from jax.experimental.pallas import tpu as pltpu
from jax.sharding import Mesh
from jax.sharding import PartitionSpec as P

HEAD_DIM = 128
GROUP = 4
CTX = ("ctx_0", "ctx_1")
GRP_CTX = ("grp", "ctx_0", "ctx_1")
MASKED = -1e30
EMPTY = -1e29
EPSILON = 1e-05
LOG2E = 1.4426950408889634
BF16, F32 = jnp.bfloat16, jnp.float32

SEGMENTS = (2, 2, 2, 1, 1)


def dot(a, b, contract):
    return lax.dot_general(a, b, (contract, ((), ())), preferred_element_type=F32)


def cost(flops, moved):
    return pl.CostEstimate(flops=flops, bytes_accessed=moved, transcendentals=0)


def whole(count):
    return [pl.BlockSpec(memory_space=pltpu.VMEM)] * count


def project_body(rows_ref, weight_ref, own_ref, sent_ref):
    part = dot(rows_ref[...], weight_ref[...], ((1,), (0,)))
    own_ref[...] = part
    sent_ref[...] = part.astype(BF16)


def project(rows, weight):
    shape = (rows.shape[0], weight.shape[1])
    return pl.pallas_call(
        project_body,
        out_shape=(jax.ShapeDtypeStruct(shape, F32), jax.ShapeDtypeStruct(shape, BF16)),
        in_specs=whole(2),
        out_specs=tuple(whole(2)),
        compiler_params=pltpu.CompilerParams(vmem_limit_bytes=16 << 20),
        cost_estimate=cost(2 * rows.shape[0] * weight.size, 2 * weight.size),
        name="project",
    )(rows, weight)


def encode_body(own_ref, peer_ref, resid_ref, grad_ref, gain_ref, kw_ref, vw_ref, kv_ref, hg_ref):
    hidden = resid_ref[...].astype(F32) + (own_ref[...] + peer_ref[...].astype(F32))
    root = jnp.sqrt(jnp.mean(hidden * hidden, axis=-1, keepdims=True) + EPSILON)
    normed = hidden / root
    gain = gain_ref[...].astype(F32)
    visual = (normed * gain).astype(BF16)
    keys = dot(visual, kw_ref[...], ((1,), (0,))).astype(BF16)
    values = dot(visual, vw_ref[...], ((1,), (0,)))
    for h in range(kv_ref.shape[0]):
        cols = slice(h * HEAD_DIM, (h + 1) * HEAD_DIM)
        kv_ref[h, 0] = keys[:, cols]
        kv_ref[h, 1] = values[:, cols].T.astype(BF16)
    upstream = grad_ref[...].astype(F32) * gain
    inner = jnp.mean(upstream * normed, axis=-1, keepdims=True)
    hg_ref[...] = ((upstream - normed * inner) / root).astype(BF16)


def encode(own, peer, resid, grad, gain, key_weight, value_weight):
    tokens, width = resid.shape
    heads = key_weight.shape[1] // HEAD_DIM
    return pl.pallas_call(
        encode_body,
        out_shape=(
            jax.ShapeDtypeStruct((heads, 2, HEAD_DIM, tokens), BF16),
            jax.ShapeDtypeStruct((tokens, width), BF16),
        ),
        in_specs=whole(7),
        out_specs=tuple(whole(2)),
        compiler_params=pltpu.CompilerParams(vmem_limit_bytes=24 << 20),
        cost_estimate=cost(4 * tokens * key_weight.size, 4 * key_weight.size),
        name="encode",
    )(own, peer, resid, grad, gain, key_weight, value_weight)


def term_body(rows_ref, hg_ref, out_ref):
    term = dot(rows_ref[...], hg_ref[...], ((0,), (0,))).astype(BF16)
    part = out_ref.shape[2]
    for d in range(out_ref.shape[0]):
        out_ref[d] = term[:, d * part : (d + 1) * part]


def weight_term(rows, hidden_grad, parts):
    shape = (parts, rows.shape[1], hidden_grad.shape[1] // parts)
    return pl.pallas_call(
        term_body,
        out_shape=jax.ShapeDtypeStruct(shape, BF16),
        in_specs=whole(2),
        out_specs=whole(1)[0],
        compiler_params=pltpu.CompilerParams(vmem_limit_bytes=16 << 20),
        cost_estimate=cost(2 * rows.size * hidden_grad.shape[1], 2 << 20),
        name="weight_term",
    )(rows, hidden_grad)


def attend_body(fresh, last, units, base_ref, lo_ref, hi_ref, q_ref, *refs):
    kv_refs = refs[: 2 * units]
    refs = refs[2 * units :]
    if fresh:
        state_refs, refs = (), refs
    else:
        state_refs, refs = refs[:2], refs[2:]
    if last:
        out_refs, (acc_ref, max_ref) = refs[:1], refs[1:]
    else:
        out_refs, (acc_ref, max_ref) = refs[:2], refs[2:]
    width = acc_ref.shape[1]
    ones_rows = acc_ref.shape[0] - HEAD_DIM
    if fresh:
        acc_ref[...] = jnp.zeros_like(acc_ref)
        max_ref[...] = jnp.full_like(max_ref, EMPTY)
    else:
        lse = state_refs[1][0]
        max_ref[...] = lse
        acc_ref[:HEAD_DIM, :] = state_refs[0][0].astype(F32)
        acc_ref[HEAD_DIM:, :] = jnp.broadcast_to(
            jnp.where(lse > 0.5 * EMPTY, 1.0, 0.0), (ones_rows, width)
        )
    q = q_ref[...]
    q = jnp.concatenate([q[:, g * HEAD_DIM : (g + 1) * HEAD_DIM] for g in range(GROUP)], axis=0)
    scale = HEAD_DIM ** (-0.5) * LOG2E
    lo_all, hi_all = lo_ref[...], hi_ref[...]
    for u in range(units):
        first, second = kv_refs[2 * u], kv_refs[2 * u + 1]
        base = (base_ref[u, 0], base_ref[u, 1])
        touched = ((lo_all < base[0] + HEAD_DIM) & (hi_all > base[0])) | (
            (lo_all < base[1] + HEAD_DIM) & (hi_all > base[1])
        )
        needed = jnp.max(jnp.where(touched, 1.0, 0.0)) > 0.0

        @pl.when(needed)
        def _():
            keys = jnp.concatenate([first[0, 0], second[0, 0]], axis=0)
            values = jnp.concatenate([first[0, 1], second[0, 1]], axis=1)
            values = jnp.concatenate([values, jnp.ones((ones_rows, 2 * HEAD_DIM), BF16)], axis=0)
            row = lax.broadcasted_iota(jnp.int32, (2 * HEAD_DIM, 1), 0)
            position = jnp.where(row < HEAD_DIM, base[0] + row, base[1] + row - HEAD_DIM)
            for at in range(0, width, 256):
                to = min(at + 256, width)
                lo, hi = lo_ref[:, at:to], hi_ref[:, at:to]
                scores = dot(keys, q[at:to], ((1,), (1,))) * scale
                scores = jnp.where((position >= lo) & (position < hi), scores, MASKED)
                old = max_ref[:, at:to]
                new = jnp.maximum(old, jnp.max(scores, axis=0, keepdims=True))
                weights = jnp.exp2(scores - new).astype(BF16)
                acc_ref[:, at:to] = acc_ref[:, at:to] * jnp.exp2(old - new) + dot(
                    values, weights, ((1,), (0,))
                )
                max_ref[:, at:to] = new

    total = acc_ref[HEAD_DIM : HEAD_DIM + 1, :]
    some = total > 0.0
    total = jnp.where(some, total, 1.0)
    mean = (acc_ref[:HEAD_DIM, :] / total).astype(BF16)
    lse = jnp.where(some, max_ref[...] + jnp.log2(total), EMPTY)
    out_refs[0][0, :HEAD_DIM, :] = mean
    if last:
        high = lse.astype(BF16)
        rest = lse - high.astype(F32)
        middle = rest.astype(BF16)
        low = (rest - middle.astype(F32)).astype(BF16)
        index = lax.broadcasted_iota(jnp.int32, (ones_rows, width), 0)
        pieces = jnp.where(index == 0, high.astype(F32), 0.0)
        pieces = jnp.where(index == 1, middle.astype(F32), pieces)
        pieces = jnp.where(index == 2, low.astype(F32), pieces)
        out_refs[0][0, HEAD_DIM:, :] = pieces.astype(BF16)
    else:
        out_refs[1][0] = lse


def attend(q, lo, hi, bases, shards, state, last):
    units = len(shards) // 2
    tokens = q.shape[0]
    width = GROUP * tokens
    heads = q.shape[1] // (GROUP * HEAD_DIM)
    tall = HEAD_DIM + 16
    row = pl.BlockSpec((1, width), lambda h: (0, 0))
    mean = pl.BlockSpec((1, HEAD_DIM, width), lambda h: (h, 0, 0))
    lse = pl.BlockSpec((1, 1, width), lambda h: (h, 0, 0))
    shard = pl.BlockSpec((1, 2, HEAD_DIM, HEAD_DIM), lambda h: (h, 0, 0, 0))
    in_specs = [
        pl.BlockSpec(memory_space=pltpu.SMEM),
        row,
        row,
        pl.BlockSpec((tokens, GROUP * HEAD_DIM), lambda h: (0, h)),
    ] + [shard] * (2 * units)
    operands = [bases, lo, hi, q, *shards]
    if state is not None:
        in_specs += [mean, lse]
        operands += list(state)
    if last:
        out_shape = [jax.ShapeDtypeStruct((heads, tall, width), BF16)]
        out_specs = [pl.BlockSpec((1, tall, width), lambda h: (h, 0, 0))]
    else:
        out_shape = [
            jax.ShapeDtypeStruct((heads, HEAD_DIM, width), BF16),
            jax.ShapeDtypeStruct((heads, 1, width), F32),
        ]
        out_specs = [mean, lse]
    out = pl.pallas_call(
        functools.partial(attend_body, state is None, last, units),
        out_shape=out_shape,
        grid=(heads,),
        in_specs=in_specs,
        out_specs=out_specs,
        scratch_shapes=[pltpu.VMEM((tall, width), F32), pltpu.VMEM((1, width), F32)],
        compiler_params=pltpu.CompilerParams(
            dimension_semantics=("arbitrary",), vmem_limit_bytes=24 << 20
        ),
        cost_estimate=cost(
            4 * units * heads * 2 * HEAD_DIM * width * HEAD_DIM, 2 * q.size + units * (512 << 10)
        ),
        name="attend",
    )(*operands)
    return out[0] if last else tuple(out)


def combine_body(mine_ref, theirs_ref, out_ref):
    def parts(ref):
        pieces = ref[0, HEAD_DIM:, :].astype(F32)
        return ref[0, :HEAD_DIM, :].astype(F32), pieces[0:1] + pieces[1:2] + pieces[2:3]

    (mean_a, lse_a), (mean_b, lse_b) = parts(mine_ref), parts(theirs_ref)
    top = jnp.maximum(lse_a, lse_b)
    weight_a, weight_b = jnp.exp2(lse_a - top), jnp.exp2(lse_b - top)
    mixed = (mean_a * weight_a + mean_b * weight_b) / (weight_a + weight_b)
    turned = mixed.T.astype(BF16)
    tokens = out_ref.shape[0]
    for g in range(GROUP):
        out_ref[:, g * HEAD_DIM : (g + 1) * HEAD_DIM] = turned[g * tokens : (g + 1) * tokens]


def combine(mine, theirs, tokens):
    heads, tall, width = mine.shape
    part = pl.BlockSpec((1, tall, width), lambda h: (h, 0, 0))
    return pl.pallas_call(
        combine_body,
        out_shape=jax.ShapeDtypeStruct((tokens, heads * GROUP * HEAD_DIM), BF16),
        grid=(heads,),
        in_specs=[part, part],
        out_specs=pl.BlockSpec((tokens, GROUP * HEAD_DIM), lambda h: (0, h)),
        compiler_params=pltpu.CompilerParams(
            dimension_semantics=("arbitrary",), vmem_limit_bytes=16 << 20
        ),
        cost_estimate=cost(8 * mine.size, 6 * mine.size),
        name="combine",
    )(mine, theirs)


def token_scene(segments, doc_scene):
    numbers = jnp.arange(doc_scene.shape[0], dtype=jnp.int32)
    picked = (segments[:, None] == numbers[None, :]).astype(jnp.int32)
    return jnp.sum(picked * doc_scene[None, :], axis=1)


def key_ranges(scene, lengths):
    count = lengths.shape[0]
    numbers = jnp.arange(count, dtype=jnp.int32)
    ends = jnp.sum(jnp.where(numbers[None, :] <= numbers[:, None], lengths[None, :], 0), axis=1)
    picked = scene[None, :] == numbers[:, None]
    hi = jnp.sum(jnp.where(picked, ends[:, None], 0), axis=0)
    lo = hi - jnp.sum(jnp.where(picked, lengths[:, None], 0), axis=0)
    return (
        jnp.tile(lo, GROUP)[None, :].astype(jnp.int32),
        jnp.tile(hi, GROUP)[None, :].astype(jnp.int32),
    )


def local(
    resid,
    attn_ctx,
    enc_out_weight,
    enc_gain,
    key_weight,
    value_weight,
    visual_grad,
    scene_lengths,
    text_queries,
    text_segments,
    doc_scene,
):
    ring = lax.axis_size("ctx_0")
    replicas = lax.axis_size("dp")
    chip, core = lax.axis_index("ctx_0"), lax.axis_index("ctx_1")
    swap = [(0, 1), (1, 0)]
    rows = attn_ctx[0]
    own_part, sent_part = project(rows, enc_out_weight)
    peer_part = lax.ppermute(sent_part, "grp", swap)

    queries = text_queries[0]
    tokens = queries.shape[0]
    scene = token_scene(text_segments[0], doc_scene[0])
    peer_queries = lax.ppermute(queries, "ctx_1", swap)
    peer_scene = lax.ppermute(scene.astype(F32), "ctx_1", swap).astype(jnp.int32)
    halves = (
        (queries, *key_ranges(scene, scene_lengths[0])),
        (peer_queries, *key_ranges(peer_scene, scene_lengths[0])),
    )

    shard, hidden_grad = encode(
        own_part, peer_part, resid[0], visual_grad[0], enc_gain[None, :], key_weight, value_weight
    )
    other = lax.ppermute(shard, "ctx_1", swap)
    block = jnp.stack([shard, other])

    pairs = []
    for z in range(ring):
        pairs.append((2 * z, 2 * ((z + 1) % ring)))
        pairs.append((2 * z + 1, 2 * ((z - 1) % ring) + 1))
    units = []
    for turn in range(1, ring // 2 + 1):
        block = lax.ppermute(block[:1] if turn == ring // 2 else block, CTX, pairs)
        source = lax.rem(jnp.where(core == 0, chip - turn, chip + turn) + ring, ring)
        here = [source * 256 + lax.rem(core + j, 2) * 128 for j in (0, 1)]
        if turn < ring // 2:
            units.append(((block[0], block[1]), here))
        else:
            units.append(((block[0], shard), [here[0], chip * 256 + core * 128]))

    term = weight_term(rows, hidden_grad, replicas)
    over_dp = lax.all_to_all(term, "dp", 0, 0, tiled=True)
    over_dp = jnp.sum(over_dp.astype(F32), axis=0).astype(BF16)
    cut = over_dp.reshape(2 * ring, -1, over_dp.shape[1])
    over_ctx = lax.all_to_all(cut, CTX, 0, 0, tiled=True)
    mine = jnp.sum(over_ctx.astype(F32), axis=0)
    columns = lax.all_to_all(
        jnp.broadcast_to(mine[None], (replicas, *mine.shape)), "dp", 0, 0, tiled=True
    )
    weight_grad = jnp.moveaxis(columns, 0, 1).reshape(mine.shape[0], -1)

    states = [None, None]
    at = 0
    scale = [s for s in SEGMENTS] if sum(SEGMENTS) == len(units) else [1] * len(units)
    for number, size in enumerate(scale):
        taken = units[at : at + size]
        at += size
        last = number == len(scale) - 1
        bases = jnp.stack([jnp.stack(u[1]) for u in taken]).astype(jnp.int32)
        shards = [s for u in taken for s in u[0]]
        for half in (1, 0):
            q, lo, hi = halves[half]
            states[half] = attend(q, lo, hi, bases, shards, states[half], last)
    theirs = lax.ppermute(states[1], "ctx_1", swap)
    context = combine(states[0], theirs, tokens)
    return (context[None], weight_grad)


def solution(mesh):
    split = Mesh(
        mesh.devices.reshape(
            mesh.shape["grp"], mesh.shape["ctx"] // 2, 2, mesh.shape["dp"]
        ),
        ("grp", "ctx_0", "ctx_1", "dp"),
    )
    placed = (
        P("dp", CTX, None),
        P("dp", CTX, "grp"),
        P("grp", None),
        P(),
        P(None, "grp"),
        P(None, "grp"),
        P("dp", CTX, None),
        P("dp", None),
        P("dp", CTX, "grp"),
        P("dp", CTX),
        P("dp", None),
    )
    return jax.shard_map(
        local,
        mesh=split,
        in_specs=placed,
        out_specs=(P("dp", CTX, "grp"), P(GRP_CTX, None)),
        check_vma=False,
    )
```

```python
import functools

import jax
import jax.numpy as jnp
from jax import lax
from jax.experimental import pallas as pl
from jax.experimental.pallas import tpu as pltpu
from jax.sharding import Mesh
from jax.sharding import PartitionSpec as P

HEAD_DIM = 128
GROUP = 4
CTX = ("ctx_0", "ctx_1")
GRP_CTX = ("grp", "ctx_0", "ctx_1")
MASKED = -1e30
EMPTY = -1e29
EPSILON = 1e-05
LOG2E = 1.4426950408889634
BF16, F32 = jnp.bfloat16, jnp.float32

BLOCK = 64


def dot(a, b, contract):
    return lax.dot_general(a, b, (contract, ((), ())), preferred_element_type=F32)


def cost(flops, moved):
    return pl.CostEstimate(flops=flops, bytes_accessed=moved, transcendentals=0)


def whole(count):
    return [pl.BlockSpec(memory_space=pltpu.VMEM)] * count


def project_body(rows_ref, weight_ref, own_ref, sent_ref):
    part = dot(rows_ref[...], weight_ref[...], ((1,), (0,)))
    own_ref[...] = part
    sent_ref[...] = part.astype(BF16)


def project(rows, weight):
    shape = (rows.shape[0], weight.shape[1])
    return pl.pallas_call(
        project_body,
        out_shape=(jax.ShapeDtypeStruct(shape, F32), jax.ShapeDtypeStruct(shape, BF16)),
        in_specs=whole(2),
        out_specs=tuple(whole(2)),
        compiler_params=pltpu.CompilerParams(vmem_limit_bytes=16 << 20),
        cost_estimate=cost(2 * rows.shape[0] * weight.size, 2 * weight.size),
        name="project",
    )(rows, weight)


def encode_body(
    own_ref, peer_ref, resid_ref, grad_ref, gain_ref, kw_hbm, vw_hbm, kv_ref, hg_ref, kw_ref, vw_ref, sems
):
    loads = (
        pltpu.make_async_copy(kw_hbm, kw_ref, sems.at[0]),
        pltpu.make_async_copy(vw_hbm, vw_ref, sems.at[1]),
    )
    for load in loads:
        load.start()
    hidden = resid_ref[...].astype(F32) + (own_ref[...] + peer_ref[...].astype(F32))
    root = jnp.sqrt(jnp.mean(hidden * hidden, axis=-1, keepdims=True) + EPSILON)
    normed = hidden / root
    gain = gain_ref[...].astype(F32)
    visual = (normed * gain).astype(BF16)
    upstream = grad_ref[...].astype(F32) * gain
    inner = jnp.mean(upstream * normed, axis=-1, keepdims=True)
    hg_ref[...] = ((upstream - normed * inner) / root).astype(BF16)
    loads[0].wait()
    keys = dot(visual, kw_ref[...], ((1,), (0,))) * (HEAD_DIM ** (-0.5) * LOG2E)
    loads[1].wait()
    values = dot(visual, vw_ref[...], ((1,), (0,)))
    for h in range(kv_ref.shape[0]):
        cols = slice(h * HEAD_DIM, (h + 1) * HEAD_DIM)
        kv_ref[h, 0] = keys[:, cols].astype(BF16)
        kv_ref[h, 1] = values[:, cols].T.astype(BF16)


def encode(own, peer, resid, grad, gain, key_weight, value_weight):
    tokens, width = resid.shape
    heads = key_weight.shape[1] // HEAD_DIM
    return pl.pallas_call(
        encode_body,
        out_shape=(
            jax.ShapeDtypeStruct((heads, 2, HEAD_DIM, tokens), BF16),
            jax.ShapeDtypeStruct((tokens, width), BF16),
        ),
        in_specs=whole(5) + [pl.BlockSpec(memory_space=pl.ANY)] * 2,
        out_specs=tuple(whole(2)),
        scratch_shapes=[
            pltpu.VMEM(key_weight.shape, BF16),
            pltpu.VMEM(value_weight.shape, BF16),
            pltpu.SemaphoreType.DMA((2,)),
        ],
        compiler_params=pltpu.CompilerParams(vmem_limit_bytes=16 << 20),
        cost_estimate=cost(4 * tokens * key_weight.size, 4 * key_weight.size),
        name="encode",
    )(own, peer, resid, grad, gain, key_weight, value_weight)


def term_body(rows_ref, hg_ref, out_ref):
    term = dot(rows_ref[...], hg_ref[...], ((0,), (0,))).astype(BF16)
    part = out_ref.shape[2]
    for d in range(out_ref.shape[0]):
        out_ref[d] = term[:, d * part : (d + 1) * part]


def weight_term(rows, hidden_grad, parts):
    shape = (parts, rows.shape[1], hidden_grad.shape[1] // parts)
    return pl.pallas_call(
        term_body,
        out_shape=jax.ShapeDtypeStruct(shape, BF16),
        in_specs=whole(2),
        out_specs=whole(1)[0],
        compiler_params=pltpu.CompilerParams(vmem_limit_bytes=16 << 20),
        cost_estimate=cost(2 * rows.size * hidden_grad.shape[1], 2 << 20),
        name="weight_term",
    )(rows, hidden_grad)


def blocks_of(tokens):
    return [(at, min(BLOCK, tokens - at)) for at in range(0, tokens, BLOCK)]


def attend_body(lengths_ref, scene_ref, q_hbm, kv_hbm, out_hbm, q_ref, kv_ref, acc_ref, out_ref, q_sem, kv_sem, out_sem):
    heads, tall, width = acc_ref.shape
    shards = kv_hbm.shape[0]
    tokens = width // GROUP
    q_load = pltpu.make_async_copy(q_hbm, q_ref, q_sem)
    q_load.start()
    scenes = lengths_ref.shape[1]
    starts, ends, end = [], [], jnp.int32(0)
    for s in range(scenes):
        starts.append(end)
        end = end + lengths_ref[0, s]
        ends.append(end)

    scene = scene_ref[...]
    seen_any = [jnp.max(jnp.where(scene == s, 1.0, 0.0)) > 0.0 for s in range(scenes)]
    lo_all, hi_all = jnp.zeros_like(scene), jnp.zeros_like(scene)
    for s in range(scenes):
        lo_all = jnp.where(scene == s, starts[s], lo_all)
        hi_all = jnp.where(scene == s, ends[s], hi_all)

    def needed(i):
        need = jnp.bool_(False)
        for s in range(scenes):
            need = need | (
                seen_any[s] & (starts[s] < (i + 1) * HEAD_DIM) & (ends[s] > i * HEAD_DIM)
            )
        return need

    def load(i):
        return pltpu.make_async_copy(kv_hbm.at[i], kv_ref.at[i], kv_sem.at[i])

    def start_one(i, carry):
        @pl.when(needed(i))
        def _():
            load(i).start()

        return carry

    def wait_one(i, carry):
        @pl.when(needed(i))
        def _():
            load(i).wait()

        return carry

    lax.fori_loop(0, shards, start_one, 0)
    kv_ref[shards] = jnp.zeros(kv_ref.shape[1:], BF16)
    q_load.wait()
    lax.fori_loop(0, shards, wait_one, 0)

    ones = jnp.ones((tall - HEAD_DIM, 2 * HEAD_DIM), BF16)
    row = lax.broadcasted_iota(jnp.int32, (2 * HEAD_DIM, 1), 0)

    for first, size in blocks_of(tokens):
        cols = slice(first * GROUP, (first + size) * GROUP)
        block_scene = scene[:, cols]
        lo, hi = lo_all[:, cols], hi_all[:, cols]
        acc_ref[:, :, cols] = jnp.zeros((heads, tall, size * GROUP), F32)
        whole_lo, whole_hi = jnp.max(lo), jnp.min(hi)
        queries = []
        for h in range(heads):
            queries.append(
                jnp.concatenate(
                    [
                        q_ref[first : first + size, (h * GROUP + g) * HEAD_DIM : (h * GROUP + g + 1) * HEAD_DIM]
                        for g in range(GROUP)
                    ],
                    axis=0,
                )
            )

        def chunk(masked, a, b, lo, hi, tops):
            keys = [jnp.concatenate([kv_ref[a, h, 0], kv_ref[b, h, 0]], axis=0) for h in range(heads)]
            scores = [dot(keys[h], queries[h], ((1,), (1,))) for h in range(heads)]
            if masked:
                position = a * HEAD_DIM + row
                allowed = (position >= lo) & (position < hi)
            new_tops = []
            for h in range(heads):
                score = jnp.where(allowed, scores[h], MASKED) if masked else scores[h]
                new = jnp.maximum(tops[h], jnp.max(score, axis=0, keepdims=True))
                weights = jnp.exp2(score - new).astype(BF16)
                values = jnp.concatenate([kv_ref[a, h, 1], kv_ref[b, h, 1]], axis=1)
                values = jnp.concatenate([values, ones], axis=0)
                acc_ref[h, :, cols] = acc_ref[h, :, cols] * jnp.exp2(tops[h] - new) + dot(
                    values, weights, ((1,), (0,))
                )
                new_tops.append(new)
            return tuple(new_tops)

        tops = tuple(jnp.full((1, size * GROUP), EMPTY, F32) for _ in range(heads))
        for s in range(scenes):
            seen = jnp.max(jnp.where(block_scene == s, 1.0, 0.0)) > 0.0
            begin = starts[s] // HEAD_DIM
            count = jnp.where(seen, (ends[s] - begin * HEAD_DIM + 2 * HEAD_DIM - 1) // (2 * HEAD_DIM), 0)

            here = block_scene == s
            lo_here, hi_here = jnp.where(here, lo, 0), jnp.where(here, hi, 0)

            def step(i, tops, begin=begin, lo=lo_here, hi=hi_here):
                a = begin + 2 * i
                at = a * HEAD_DIM
                inside = (at >= whole_lo) & (at + 2 * HEAD_DIM <= whole_hi)
                b = a + 1
                b = jnp.where(needed(b), b, shards)
                return lax.cond(
                    inside,
                    lambda t: chunk(False, a, b, lo, hi, t),
                    lambda t: chunk(True, a, b, lo, hi, t),
                    tops,
                )

            tops = lax.fori_loop(0, count, step, tops)

        for h in range(heads):
            total = acc_ref[h, HEAD_DIM : HEAD_DIM + 1, cols]
            mean = acc_ref[h, :HEAD_DIM, cols] * (1.0 / total)
            turned = mean.T.astype(BF16)
            for g in range(GROUP):
                out_ref[
                    first : first + size,
                    (h * GROUP + g) * HEAD_DIM : (h * GROUP + g + 1) * HEAD_DIM,
                ] = turned[g * size : (g + 1) * size]

    out_copy = pltpu.make_async_copy(out_ref, out_hbm, out_sem)
    out_copy.start()
    out_copy.wait()


def attend(lengths, scene, q, kv):
    tokens, features = q.shape
    heads = kv.shape[1]
    width = GROUP * tokens
    tall = HEAD_DIM + 16
    anywhere = pl.BlockSpec(memory_space=pl.ANY)
    return pl.pallas_call(
        attend_body,
        out_shape=jax.ShapeDtypeStruct(q.shape, BF16),
        in_specs=[pl.BlockSpec(memory_space=pltpu.SMEM), *whole(1), anywhere, anywhere],
        out_specs=anywhere,
        scratch_shapes=[
            pltpu.VMEM(q.shape, BF16),
            pltpu.VMEM((kv.shape[0] + 1, *kv.shape[1:]), BF16),
            pltpu.VMEM((heads, tall, width), F32),
            pltpu.VMEM(q.shape, BF16),
            pltpu.SemaphoreType.DMA(()),
            pltpu.SemaphoreType.DMA((kv.shape[0],)),
            pltpu.SemaphoreType.DMA(()),
        ],
        compiler_params=pltpu.CompilerParams(vmem_limit_bytes=32 << 20),
        cost_estimate=cost(4 * q.size * 1024, 4 * q.size + kv.size),
        name="attend",
    )(lengths, scene, q, kv)


def token_scene(segments, doc_scene):
    numbers = jnp.arange(doc_scene.shape[0], dtype=jnp.int32)
    picked = (segments[:, None] == numbers[None, :]).astype(jnp.int32)
    return jnp.sum(picked * doc_scene[None, :], axis=1)


def local(
    resid,
    attn_ctx,
    enc_out_weight,
    enc_gain,
    key_weight,
    value_weight,
    visual_grad,
    scene_lengths,
    text_queries,
    text_segments,
    doc_scene,
):
    ring = lax.axis_size("ctx_0")
    replicas = lax.axis_size("dp")
    chip, core = lax.axis_index("ctx_0"), lax.axis_index("ctx_1")
    swap = [(0, 1), (1, 0)]
    rows = attn_ctx[0]
    own_part, sent_part = project(rows, enc_out_weight)
    peer_part = lax.ppermute(sent_part, "grp", swap)

    shard, hidden_grad = encode(
        own_part, peer_part, resid[0], visual_grad[0], enc_gain[None, :], key_weight, value_weight
    )
    gathered = lax.all_gather(shard[None], CTX, axis=0, tiled=True)

    queries = text_queries[0]
    tokens = queries.shape[0]
    scene = token_scene(text_segments[0], doc_scene[0])
    columns = [
        jnp.tile(scene[first : first + size], GROUP) for first, size in blocks_of(tokens)
    ]
    context = attend(scene_lengths, jnp.concatenate(columns)[None, :], queries, gathered)

    term = weight_term(rows, hidden_grad, replicas)
    over_dp = lax.all_to_all(term, "dp", 0, 0, tiled=True)
    total = jnp.sum(over_dp.astype(F32), axis=0)
    total = total.reshape(ring, 2, -1, total.shape[1])
    kept = lax.dynamic_index_in_dim(total, core, 1, keepdims=False)
    given = lax.dynamic_index_in_dim(total, 1 - core, 1, keepdims=False)
    total = kept + lax.ppermute(given.astype(BF16), "ctx_1", swap).astype(F32)
    reach = ring // 2
    while reach:
        bit = lax.rem(chip // reach, 2)
        kept = lax.dynamic_slice_in_dim(total, bit * reach, reach, 0)
        given = lax.dynamic_slice_in_dim(total, (1 - bit) * reach, reach, 0)
        pairs = [(z, z ^ reach) for z in range(ring)]
        total = kept + lax.ppermute(given.astype(BF16), "ctx_0", pairs).astype(F32)
        reach //= 2
    mine = total[0]
    columns = lax.all_to_all(
        jnp.broadcast_to(mine[None], (replicas, *mine.shape)), "dp", 0, 0, tiled=True
    )
    weight_grad = jnp.moveaxis(columns, 0, 1).reshape(mine.shape[0], -1)

    return (context[None], weight_grad)


def solution(mesh):
    split = Mesh(
        mesh.devices.reshape(
            mesh.shape["grp"], mesh.shape["ctx"] // 2, 2, mesh.shape["dp"]
        ),
        ("grp", "ctx_0", "ctx_1", "dp"),
    )
    placed = (
        P("dp", CTX, None),
        P("dp", CTX, "grp"),
        P("grp", None),
        P(),
        P(None, "grp"),
        P(None, "grp"),
        P("dp", CTX, None),
        P("dp", None),
        P("dp", CTX, "grp"),
        P("dp", CTX),
        P("dp", None),
    )
    return jax.shard_map(
        local,
        mesh=split,
        in_specs=placed,
        out_specs=(P("dp", CTX, "grp"), P(GRP_CTX, None)),
        check_vma=False,
    )
```

```python
import functools

import jax
import jax.numpy as jnp
from jax import lax
from jax.experimental import pallas as pl
from jax.experimental.pallas import tpu as pltpu
from jax.sharding import Mesh
from jax.sharding import PartitionSpec as P

HEAD_DIM = 128
GROUP = 4
CTX = ("ctx_0", "ctx_1")
GRP_CTX = ("grp", "ctx_0", "ctx_1")
MASKED = -1e30
EMPTY = -1e29
EPSILON = 1e-05
LOG2E = 1.4426950408889634
BF16, F32 = jnp.bfloat16, jnp.float32

BLOCK = 80
STEP = 4


def dot(a, b, contract):
    return lax.dot_general(a, b, (contract, ((), ())), preferred_element_type=F32)


def cost(flops, moved):
    return pl.CostEstimate(flops=flops, bytes_accessed=moved, transcendentals=0)


def whole(count):
    return [pl.BlockSpec(memory_space=pltpu.VMEM)] * count


def project_body(rows_hbm, weight_hbm, own_ref, sent_ref, rows_ref, weight_ref, sems):
    loads = (
        pltpu.make_async_copy(weight_hbm, weight_ref, sems.at[0]),
        pltpu.make_async_copy(rows_hbm, rows_ref, sems.at[1]),
    )
    for load in loads:
        load.start()
    for load in loads:
        load.wait()
    part = dot(rows_ref[...], weight_ref[...], ((1,), (0,)))
    own_ref[...] = part
    sent_ref[...] = part.astype(BF16)


def project(rows, weight):
    shape = (rows.shape[0], weight.shape[1])
    return pl.pallas_call(
        project_body,
        out_shape=(jax.ShapeDtypeStruct(shape, F32), jax.ShapeDtypeStruct(shape, BF16)),
        in_specs=[pl.BlockSpec(memory_space=pl.ANY)] * 2,
        out_specs=tuple(whole(2)),
        scratch_shapes=[
            pltpu.VMEM(rows.shape, BF16),
            pltpu.VMEM(weight.shape, BF16),
            pltpu.SemaphoreType.DMA((2,)),
        ],
        compiler_params=pltpu.CompilerParams(vmem_limit_bytes=56 << 20),
        cost_estimate=cost(2 * rows.shape[0] * weight.size, 2 * weight.size),
        name="project",
    )(rows, weight)


def preload_body(count, after_hbm, *refs):
    sources, targets, sems = refs[:count], refs[count : 2 * count], refs[2 * count]
    loads = [
        pltpu.make_async_copy(sources[i], targets[i], sems.at[i]) for i in range(count)
    ]
    for load in loads:
        load.start()
    for load in loads:
        load.wait()


def preload(after, *arrays):
    count = len(arrays)
    return pl.pallas_call(
        functools.partial(preload_body, count),
        out_shape=tuple(pltpu.VMEM(a.shape, a.dtype) for a in arrays),
        in_specs=[pl.BlockSpec(memory_space=pl.ANY)] * (count + 1),
        out_specs=tuple(whole(count)),
        scratch_shapes=[pltpu.SemaphoreType.DMA((count,))],
        compiler_params=pltpu.CompilerParams(vmem_limit_bytes=8 << 20),
        cost_estimate=cost(256 << 20, sum(a.size for a in arrays) * 4),
        name="preload",
    )(after, *arrays)


def encode_body(own_ref, peer_ref, gain_ref, resid_ref, grad_ref, kw_ref, vw_ref, kv_ref, hg_ref):
    hidden = resid_ref[...].astype(F32) + (own_ref[...] + peer_ref[...].astype(F32))
    root = jnp.sqrt(jnp.mean(hidden * hidden, axis=-1, keepdims=True) + EPSILON)
    normed = hidden / root
    gain = gain_ref[...].astype(F32)
    visual = (normed * gain).astype(BF16)
    upstream = grad_ref[...].astype(F32) * gain
    inner = jnp.mean(upstream * normed, axis=-1, keepdims=True)
    hg_ref[...] = ((upstream - normed * inner) / root).astype(BF16)
    keys = dot(visual, kw_ref[...], ((1,), (0,))) * (HEAD_DIM ** (-0.5) * LOG2E)
    values = dot(visual, vw_ref[...], ((1,), (0,)))
    for h in range(kv_ref.shape[0]):
        cols = slice(h * HEAD_DIM, (h + 1) * HEAD_DIM)
        kv_ref[h, 0] = keys[:, cols].T.astype(BF16)
        kv_ref[h, 1] = values[:, cols].astype(BF16)


def encode(own, peer, resid, grad, gain, key_weight, value_weight):
    tokens, width = resid.shape
    heads = key_weight.shape[1] // HEAD_DIM
    return pl.pallas_call(
        encode_body,
        out_shape=(
            jax.ShapeDtypeStruct((heads, 2, HEAD_DIM, tokens), BF16),
            jax.ShapeDtypeStruct((tokens, width), BF16),
        ),
        in_specs=whole(7),
        out_specs=tuple(whole(2)),
        compiler_params=pltpu.CompilerParams(vmem_limit_bytes=16 << 20),
        cost_estimate=cost(4 * tokens * key_weight.size, 4 * key_weight.size),
        name="encode",
    )(own, peer, gain, resid, grad, key_weight, value_weight)


def term_body(rows_ref, hg_ref, out_ref):
    term = dot(rows_ref[...], hg_ref[...], ((0,), (0,))).astype(BF16)
    part = out_ref.shape[2]
    for d in range(out_ref.shape[0]):
        out_ref[d] = term[:, d * part : (d + 1) * part]


def weight_term(rows, hidden_grad, parts):
    shape = (parts, rows.shape[1], hidden_grad.shape[1] // parts)
    return pl.pallas_call(
        term_body,
        out_shape=jax.ShapeDtypeStruct(shape, BF16),
        in_specs=whole(2),
        out_specs=whole(1)[0],
        compiler_params=pltpu.CompilerParams(vmem_limit_bytes=16 << 20),
        cost_estimate=cost(2 * rows.size * hidden_grad.shape[1], 2 << 20),
        name="weight_term",
    )(rows, hidden_grad)


def blocks_of(tokens):
    size = BLOCK if tokens % BLOCK == 0 else tokens
    return [(at, size) for at in range(0, tokens, size)]


def attend_body(
    lengths_ref, scene_ref, q_hbm, kv_hbm, out_hbm,
    q_ref, kv_ref, acc_ref, top_ref, out_ref, plan_ref, ready_ref, q_sem, kv_sem, out_sem,
):
    heads, height, wide = acc_ref.shape
    shards = kv_hbm.shape[0]
    scenes = lengths_ref.shape[1]
    size = height // GROUP
    q_load = pltpu.make_async_copy(q_hbm, q_ref, q_sem)
    q_load.start()

    def load(begin, slot):
        return pltpu.make_async_copy(
            kv_hbm.at[pl.ds(begin, STEP)], kv_ref.at[pl.ds(slot * STEP, STEP)], kv_sem.at[slot]
        )

    scene = scene_ref[...]
    end, slots = jnp.int32(0), jnp.int32(0)
    for s in range(scenes):
        start, end = end, end + lengths_ref[0, s]
        seen = jnp.max(jnp.where(scene == s, 1.0, 0.0)) > 0.0
        begin = start // HEAD_DIM
        count = (end - begin * HEAD_DIM + STEP * HEAD_DIM - 1) // (STEP * HEAD_DIM)
        count = jnp.where(seen, count, 0)
        begin = jnp.minimum(begin, shards - count * STEP)
        for k, value in enumerate((start, end, begin, count, slots)):
            plan_ref[s, k] = value

        def start_one(i, carry, begin=begin, slots=slots):
            load(begin + i * STEP, slots + i).start()
            ready_ref[slots + i] = 0
            return carry

        lax.fori_loop(0, count, start_one, 0)
        slots = slots + count
    q_load.wait()

    ones = jnp.ones((STEP * HEAD_DIM, wide - HEAD_DIM), BF16)
    column = lax.broadcasted_iota(jnp.int32, (1, STEP * HEAD_DIM), 1)

    def block(b, carry):
        row = pl.multiple_of(b * height, height)
        first = pl.multiple_of(b * size, size)
        own = scene_ref[pl.ds(row, height), :]
        acc_ref[...] = jnp.zeros_like(acc_ref)
        top_ref[...] = jnp.full_like(top_ref, EMPTY)

        def one_scene(s, carry):
            start, end, begin, count, slot = [plan_ref[s, k] for k in range(5)]
            share = jnp.where(own == s, 1.0, 0.0)
            seen, alone = jnp.max(share) > 0.0, jnp.min(share) > 0.0
            lo = jnp.where(own == s, start, 0)
            hi = jnp.where(own == s, end, 0)

            def step(i, carry):
                at = slot + i
                key = (begin + i * STEP) * HEAD_DIM
                base = at * STEP

                @pl.when(ready_ref[at] == 0)
                def _():
                    load(begin + i * STEP, at).wait()
                    ready_ref[at] = 1

                def take(masked):
                    if masked:
                        position = key + column
                        allowed = (position >= lo) & (position < hi)
                    for h in range(heads):
                        parts = []
                        for g in range(GROUP):
                            col = (h * GROUP + g) * HEAD_DIM
                            parts.append(q_ref[pl.ds(first, size), col : col + HEAD_DIM])
                        queries = jnp.concatenate(parts, axis=0)
                        keys = jnp.concatenate([kv_ref[base + j, h, 0] for j in range(STEP)], axis=1)
                        score = dot(queries, keys, ((1,), (0,)))
                        if masked:
                            score = jnp.where(allowed, score, MASKED)
                        old = top_ref[h]
                        new = jnp.maximum(old, jnp.max(score, axis=1, keepdims=True))
                        top_ref[h] = new
                        weights = jnp.exp2(score - jnp.concatenate([new] * STEP, axis=1)).astype(BF16)
                        values = jnp.concatenate([kv_ref[base + j, h, 1] for j in range(STEP)], axis=0)
                        values = jnp.concatenate([values, ones], axis=1)
                        fade = jnp.exp2(old - new)
                        acc_ref[h] = acc_ref[h] * jnp.concatenate([fade, fade], axis=1) + dot(
                            weights, values, ((1,), (0,))
                        )

                inside = alone & (key >= start) & (key + STEP * HEAD_DIM <= end)

                @pl.when(inside)
                def _():
                    take(False)

                @pl.when(jnp.logical_not(inside))
                def _():
                    take(True)

                return carry

            lax.fori_loop(0, jnp.where(seen, count, 0), step, 0)
            return carry

        lax.fori_loop(0, scenes, one_scene, 0)
        for h in range(heads):
            mean = acc_ref[h, :, :HEAD_DIM] / acc_ref[h, :, HEAD_DIM:]
            for g in range(GROUP):
                col = (h * GROUP + g) * HEAD_DIM
                out_ref[pl.ds(first, size), col : col + HEAD_DIM] = mean[
                    g * size : (g + 1) * size
                ].astype(BF16)
        return carry

    lax.fori_loop(0, q_ref.shape[0] // size, block, 0)
    out_copy = pltpu.make_async_copy(out_ref, out_hbm, out_sem)
    out_copy.start()
    out_copy.wait()


def attend(lengths, scene, q, kv):
    tokens, features = q.shape
    heads = kv.shape[1]
    size = blocks_of(tokens)[0][1]
    height = GROUP * size
    slots = kv.shape[0] // STEP + 2 * lengths.shape[1]
    anywhere = pl.BlockSpec(memory_space=pl.ANY)
    return pl.pallas_call(
        attend_body,
        out_shape=jax.ShapeDtypeStruct(q.shape, BF16),
        in_specs=[pl.BlockSpec(memory_space=pltpu.SMEM), *whole(1), anywhere, anywhere],
        out_specs=anywhere,
        scratch_shapes=[
            pltpu.VMEM(q.shape, BF16),
            pltpu.VMEM((slots * STEP, *kv.shape[1:]), BF16),
            pltpu.VMEM((heads, height, 2 * HEAD_DIM), F32),
            pltpu.VMEM((heads, height, HEAD_DIM), F32),
            pltpu.VMEM(q.shape, BF16),
            pltpu.SMEM((lengths.shape[1], 5), jnp.int32),
            pltpu.SMEM((slots,), jnp.int32),
            pltpu.SemaphoreType.DMA(()),
            pltpu.SemaphoreType.DMA((slots,)),
            pltpu.SemaphoreType.DMA(()),
        ],
        compiler_params=pltpu.CompilerParams(vmem_limit_bytes=60 << 20),
        cost_estimate=cost(4 * q.size * 1024, 4 * q.size + kv.size),
        name="attend",
    )(lengths, scene, q, kv)


def token_scene(segments, doc_scene):
    numbers = jnp.arange(doc_scene.shape[0], dtype=jnp.int32)
    picked = (segments[:, None] == numbers[None, :]).astype(jnp.int32)
    return jnp.sum(picked * doc_scene[None, :], axis=1)


def local(
    resid,
    attn_ctx,
    enc_out_weight,
    enc_gain,
    key_weight,
    value_weight,
    visual_grad,
    scene_lengths,
    text_queries,
    text_segments,
    doc_scene,
):
    ring = lax.axis_size("ctx_0")
    replicas = lax.axis_size("dp")
    chip, core = lax.axis_index("ctx_0"), lax.axis_index("ctx_1")
    swap = [(0, 1), (1, 0)]
    rows = attn_ctx[0]
    own_part, sent_part = project(rows, enc_out_weight)
    peer_part = lax.ppermute(sent_part, "grp", swap)

    ahead = preload(sent_part, resid[0], visual_grad[0], key_weight, value_weight)
    shard, hidden_grad = encode(own_part, peer_part, *ahead[:2], enc_gain[None, :], *ahead[2:])
    gathered = lax.all_gather(shard[None], CTX, axis=0, tiled=True)

    queries = text_queries[0]
    tokens = queries.shape[0]
    scene = token_scene(text_segments[0], doc_scene[0])
    columns = [
        jnp.tile(scene[first : first + size], GROUP) for first, size in blocks_of(tokens)
    ]
    context = attend(scene_lengths, jnp.concatenate(columns)[:, None], queries, gathered)

    term = weight_term(rows, hidden_grad, replicas)
    over_dp = lax.all_to_all(term, "dp", 0, 0, tiled=True)
    total = jnp.sum(over_dp.astype(F32), axis=0)
    total = total.reshape(ring, 2, -1, total.shape[1])
    kept = lax.dynamic_index_in_dim(total, core, 1, keepdims=False)
    given = lax.dynamic_index_in_dim(total, 1 - core, 1, keepdims=False)
    total = kept + lax.ppermute(given.astype(BF16), "ctx_1", swap).astype(F32)
    reach = ring // 2
    while reach:
        bit = lax.rem(chip // reach, 2)
        kept = lax.dynamic_slice_in_dim(total, bit * reach, reach, 0)
        given = lax.dynamic_slice_in_dim(total, (1 - bit) * reach, reach, 0)
        pairs = [(z, z ^ reach) for z in range(ring)]
        total = kept + lax.ppermute(given.astype(BF16), "ctx_0", pairs).astype(F32)
        reach //= 2
    mine = total[0]
    columns = lax.all_to_all(
        jnp.broadcast_to(mine[None], (replicas, *mine.shape)), "dp", 0, 0, tiled=True
    )
    weight_grad = jnp.moveaxis(columns, 0, 1).reshape(mine.shape[0], -1)

    return (context[None], weight_grad)


def solution(mesh):
    split = Mesh(
        mesh.devices.reshape(
            mesh.shape["grp"], mesh.shape["ctx"] // 2, 2, mesh.shape["dp"]
        ),
        ("grp", "ctx_0", "ctx_1", "dp"),
    )
    placed = (
        P("dp", CTX, None),
        P("dp", CTX, "grp"),
        P("grp", None),
        P(),
        P(None, "grp"),
        P(None, "grp"),
        P("dp", CTX, None),
        P("dp", None),
        P("dp", CTX, "grp"),
        P("dp", CTX),
        P("dp", None),
    )
    return jax.shard_map(
        local,
        mesh=split,
        in_specs=placed,
        out_specs=(P("dp", CTX, "grp"), P(GRP_CTX, None)),
        check_vma=False,
    )
```
